32 devices in a mesh: elem: 16 (over z, y, core), band: 2 (over x).
Axes of the slice: x: 2, y: 2, z: 4, core: 2. Of those that a mesh axis runs over, the one named last changes fastest.
Arguments:
- y_current: bfloat16 [512, 64, 512], P('elem', None, 'band'), may hold values from -6 to 6
- y_previous: bfloat16 [512, 64, 512], P('elem', None, 'band'), may hold values from -6 to 6
- h_blocks: bfloat16 [512, 64, 320], P('elem'), may hold values from -0.3125 to 0.3125
- basis_sizes: int32 [512], P('elem'), may hold values from 40 to 64
- neighbours: int32 [512, 4], P('elem'), may hold values from 0 to 511, as said below
Outputs:
- filtered: bfloat16 [512, 64, 512], P('elem', None, 'band')
- margin: float32 [512, 512], P('elem', 'band')
The draws below stay inside these ranges and needn't reach their ends.
Inputs may be any that keep to these rules, and one draw needn't show every extreme that they name: `neighbours`: the elements lie on a periodic grid of 32 x 16; row i lists the elements that share an edge with element i, in the order previous grid row, next grid row, previous column, next column, so adjacency is symmetric. Element g belongs to index g // 32 of elem, whose elements fill 2 consecutive grid rows in some order; a neighbour therefore belongs to the same index or to one of the two beside it, periodically, and exactly 16 of an index's elements have a neighbour on the next index, and 16 on the previous one.
All inputs are finite; a program needn't handle non-finite values.
Results may differ from the reference program's by a relative error of at most 0.018.
Values may be sent and summed in bfloat16 or wider, within the bound.
No kernel may reach another device: no remote copies, remote signals or barrier semaphores. Data moves between devices by JAX's collectives and lax.ppermute only.
A program may use at most 64 MiB of HBM per device.

```python
import jax
import jax.numpy as jnp
from jax import lax

BMAX = 64
SX = 2
GY = 16
BD = 256
DEGREES = 2
EL_DEV = 32
ELEMS = 512
NBAND = 512
N_ELEM = 16
N_BAND = 2


def draw_neighbours(key, part):
    keys = jax.random.split(jax.random.fold_in(key, 7), N_ELEM)

    def one_order(single):
        return jax.random.permutation(single, EL_DEV)
    orders = jax.vmap(one_order)(keys).astype(jnp.int32)
    owners = jnp.arange(N_ELEM, dtype=jnp.int32)[:, None] * EL_DEV
    grid = (owners + orders).reshape(SX * N_ELEM, GY)
    upper = jnp.roll(grid, 1, axis=0)
    lower = jnp.roll(grid, -1, axis=0)
    left_side = jnp.roll(grid, 1, axis=1)
    right_side = jnp.roll(grid, -1, axis=1)
    table = jnp.stack([upper, lower, left_side, right_side], axis=-1).reshape(-1, 4)
    return jnp.zeros((ELEMS, 4), jnp.int32).at[grid.reshape(-1)].set(table)


def with_ends(array, own_key, least, high):
    extent = array.shape
    place = [jax.random.randint(jax.random.fold_in(own_key, axis), (), 0, extent[axis]) for axis in range(len(extent))]
    array = array.at[tuple(place)].set(least)
    longest = extent.index(max(extent))
    place[longest] = (place[longest] + 1) % extent[longest]
    return array.at[tuple(place)].set(high)


def level_of(own_key, dims, cuts, smallest, top_value):
    def one(axis_at, parts):
        draws = jax.random.uniform(jax.random.fold_in(jax.random.fold_in(own_key, 6), axis_at), (parts,), jnp.float32, smallest / len(cuts), top_value / len(cuts))
        return jnp.repeat(jnp.exp(draws), dims[axis_at] // parts).reshape((-1,) + (1,) * (len(dims) - axis_at - 1))

    loudness = one(*cuts[0])
    for cut in cuts[1:]:
        loudness = loudness * one(*cut)
    return loudness


def bell_draw(key, dims, width, reach, cuts=(), held_as=jnp.bfloat16):
    drawn = width * jax.random.normal(key, dims, jnp.float32)
    if cuts:
        drawn = drawn * level_of(key, dims, cuts, -0.22, 0.18)
    return jnp.clip(drawn, -reach, reach).astype(held_as)


def setup_inputs(seed: int = 0) -> dict:
    key_list = jax.random.split(jax.random.key(seed), 6)
    y_current = bell_draw(key_list[0], (ELEMS, BMAX, NBAND), 1.0, 6.0, ((0, 16), (2, 2)))
    y_previous = bell_draw(key_list[1], (ELEMS, BMAX, NBAND), 1.0, 6.0, ((0, 16), (2, 2)))
    h_blocks = bell_draw(key_list[2], (ELEMS, BMAX, 5 * BMAX), (5 * BMAX) ** -0.5, 0.3125, ((0, 16),))
    basis_sizes = with_ends(jax.random.randint(key_list[3], (ELEMS,), BMAX * 5 // 8, BMAX + 1), jax.random.fold_in(key_list[3], 1), BMAX * 5 // 8, BMAX).astype(jnp.int32)
    neighbours = draw_neighbours(jax.random.fold_in(key_list[5], 71), 0)
    return dict(y_current=y_current, y_previous=y_previous, h_blocks=h_blocks, basis_sizes=basis_sizes, neighbours=neighbours)


center_value = 0.3
spectral_half = 1.7


def filter_block(pair, h_blocks, neighbours, row_mask):
    current, previous = pair
    current = current * row_mask
    previous = previous * row_mask
    hmatrix = h_blocks.astype(jnp.float32)
    mask_float = row_mask.astype(jnp.float32)
    for degree in range(DEGREES):
        nearby = current[neighbours]
        stacked = jnp.concatenate([current[:, None], nearby], axis=1)
        stacked = stacked.reshape(current.shape[0], 5 * BMAX, current.shape[2]).astype(jnp.float32)
        applied = jnp.einsum("irc,icb->irb", hmatrix, stacked, precision=lax.Precision.HIGHEST)
        following = mask_float * ((2.0 / spectral_half) * (applied - center_value * current.astype(jnp.float32)) - previous.astype(jnp.float32))
        previous = current
        current = following.astype(jnp.bfloat16)
    return current


def reference(y_current, y_previous, h_blocks, basis_sizes, neighbours):
    row_mask = (jnp.arange(BMAX, dtype=jnp.int32)[None, :] < basis_sizes[:, None]).astype(jnp.bfloat16)[:, :, None]

    def split_bands(values):
        return values.reshape(ELEMS, BMAX, N_BAND, BD).transpose(2, 0, 1, 3)

    def run_block(pair):
        return filter_block(pair, h_blocks, neighbours, row_mask)

    blocks = lax.map(run_block, (split_bands(y_current), split_bands(y_previous)))
    filtered = blocks.transpose(1, 2, 0, 3).reshape(ELEMS, BMAX, NBAND)
    flat = filtered.reshape(ELEMS * BMAX, NBAND).astype(jnp.float32)
    margin = jnp.dot(flat.T, flat, precision=lax.Precision.HIGHEST, preferred_element_type=jnp.float32)
    margin = margin / jnp.float32(ELEMS * BMAX)
    return filtered, margin
```

```python
import jax
import jax.numpy as jnp
from jax import lax
from jax.experimental import pallas as pl
from jax.experimental.pallas import tpu as pltpu
from jax.sharding import PartitionSpec as P

GY = 16
DEGREES = 2

center_value = 0.3
spectral_half = 1.7

VM = pl.BlockSpec(memory_space=pltpu.VMEM)
SM = pl.BlockSpec(memory_space=pltpu.SMEM)


def shifted(block, axis, distance):
    count = lax.axis_size(axis)
    return lax.ppermute(block, axis, [((i - distance) % count, i) for i in range(count)])


def own_bases(local_count, count_elem):
    myself = lax.axis_index("elem")
    before = jnp.where(myself == 0, count_elem - 1, myself - 1)
    after = jnp.where(myself == count_elem - 1, 0, myself + 1)
    return before * local_count, myself * local_count, after * local_count


def within(value, base, local_count):
    return (value >= base) & (value < base + local_count)


def send_lists(near, orders, local_count, bases):
    base_prev, _, base_next = bases
    to_next = jnp.int32(0)
    to_prev = jnp.int32(0)
    for i in range(local_count):
        lower = within(near[i, 1], base_next, local_count)
        upper = within(near[i, 0], base_prev, local_count)
        orders[jnp.where(lower, to_next, 2 * GY)] = i
        orders[jnp.where(upper, GY + to_prev, 2 * GY)] = i
        to_next = to_next + lower.astype(jnp.int32)
        to_prev = to_prev + upper.astype(jnp.int32)


def row_index(block, width):
    return lax.broadcasted_iota(jnp.int32, (block, width), 0)


def pack(values, sizes, near, count_elem):
    local_count, block, width = values.shape

    def body(near, sizes, values, to_next, to_prev, orders):
        bases = own_bases(local_count, count_elem)
        send_lists(near, orders, local_count, bases)
        rows = row_index(block, width)
        for s in range(GY):
            for out, at in ((to_next, orders[s]), (to_prev, orders[GY + s])):
                held = values[at].astype(jnp.float32)
                out[s] = jnp.where(rows < sizes[at], held, 0.0).astype(jnp.bfloat16)

    halo = jax.ShapeDtypeStruct((GY, block, width), jnp.bfloat16)
    return pl.pallas_call(
        body,
        name="pack",
        in_specs=[SM, SM, VM],
        out_specs=[VM, VM],
        out_shape=[halo, halo],
        scratch_shapes=[pltpu.SMEM((2 * GY + 1,), jnp.int32)],
    )(near, sizes, values)


def tables(near, count_elem):
    local_count = near.shape[0]

    def body(near, pool_index, orders, slots, marks):
        bases = own_bases(local_count, count_elem)
        base_prev, base, base_next = bases
        send_lists(near, orders, local_count, bases)
        for j in range(2 * local_count):
            marks[j] = 0
        for i in range(local_count):
            upper = within(near[i, 0], base_prev, local_count)
            lower = within(near[i, 1], base_next, local_count)
            marks[jnp.where(upper, near[i, 0] - base_prev, 2 * local_count)] = 1
            marks[jnp.where(lower, local_count + near[i, 1] - base_next, 2 * local_count)] = 1
        from_prev = jnp.int32(local_count)
        from_next = jnp.int32(local_count + GY)
        for j in range(local_count):
            slots[j] = from_prev
            slots[local_count + j] = from_next
            from_prev = from_prev + marks[j]
            from_next = from_next + marks[local_count + j]
        for i in range(local_count):
            upper = within(near[i, 0], base_prev, local_count)
            lower = within(near[i, 1], base_next, local_count)
            far_prev = slots[jnp.where(upper, near[i, 0] - base_prev, 0)]
            far_next = slots[jnp.where(lower, local_count + near[i, 1] - base_next, 0)]
            pool_index[4 * i] = jnp.where(upper, far_prev, near[i, 0] - base)
            pool_index[4 * i + 1] = jnp.where(lower, far_next, near[i, 1] - base)
            pool_index[4 * i + 2] = near[i, 2] - base
            pool_index[4 * i + 3] = near[i, 3] - base

    return pl.pallas_call(
        body,
        name="tables",
        in_specs=[SM],
        out_specs=[SM, SM],
        out_shape=[
            jax.ShapeDtypeStruct((4 * local_count,), jnp.int32),
            jax.ShapeDtypeStruct((2 * GY + 1,), jnp.int32),
        ],
        scratch_shapes=[
            pltpu.SMEM((2 * local_count,), jnp.int32),
            pltpu.SMEM((2 * local_count + 1,), jnp.int32),
        ],
    )(near)


def degree_step(pool_index, orders, sizes, current, previous, from_prev, from_next, h_blocks, last):
    local_count, block, width = current.shape

    def body(pool_index, orders, sizes, current, previous, from_prev, from_next, h_blocks, following, *rest):
        pool = rest[-1]
        rows = row_index(block, width)
        for i in range(local_count):
            held = current[i].astype(jnp.float32)
            pool[i] = jnp.where(rows < sizes[i], held, 0.0).astype(jnp.bfloat16)
        pool[local_count : local_count + GY] = from_prev[...]
        pool[local_count + GY :] = from_next[...]
        for i in range(local_count):
            own = pool[i]
            stacked = jnp.concatenate(
                [own] + [pool[pool_index[4 * i + k]] for k in range(4)], axis=0
            )
            applied = jnp.dot(h_blocks[i], stacked, preferred_element_type=jnp.float32)
            value = 2.0 / spectral_half * (
                applied - center_value * own.astype(jnp.float32)
            ) - previous[i].astype(jnp.float32)
            following[i] = jnp.where(rows < sizes[i], value, 0.0).astype(jnp.bfloat16)
        if not last:
            to_next, to_prev = rest[:2]
            for s in range(GY):
                to_next[s] = following[orders[s]]
                to_prev[s] = following[orders[GY + s]]

    whole = jax.ShapeDtypeStruct(current.shape, jnp.bfloat16)
    halo = jax.ShapeDtypeStruct((GY, block, width), jnp.bfloat16)
    outs = [whole] if last else [whole, halo, halo]
    return pl.pallas_call(
        body,
        name="degree_last" if last else "degree",
        in_specs=[SM, SM, SM] + [VM] * 5,
        out_specs=[VM] * len(outs),
        out_shape=outs,
        scratch_shapes=[pltpu.VMEM((local_count + 2 * GY, block, width), jnp.bfloat16)],
    )(pool_index, orders, sizes, current, previous, from_prev, from_next, h_blocks)


def gram(left, right):
    return lax.dot_general(
        left, right, (((0,), (0,)), ((), ())), preferred_element_type=jnp.float32
    ).astype(jnp.bfloat16)


def on_device(y_current, y_previous, h_blocks, basis_sizes, neighbours):
    local_count, block, band_width = y_current.shape
    count_elem = lax.axis_size("elem")
    count_band = lax.axis_size("band")
    current, previous = y_current, y_previous
    to_next, to_prev = pack(current, basis_sizes, neighbours, count_elem)
    pool_index, orders = tables(neighbours, count_elem)
    for degree in range(DEGREES):
        from_prev = shifted(to_next, "elem", 1)
        from_next = shifted(to_prev, "elem", -1)
        last = degree == DEGREES - 1
        result = degree_step(
            pool_index, orders, basis_sizes, current, previous, from_prev, from_next, h_blocks, last
        )
        previous = current
        current = result[0]
        if not last:
            to_next, to_prev = result[1:]
    flat = current.reshape(local_count * block, band_width)
    band = lax.axis_index("band")
    parts = [gram(flat, flat)]
    for step in range(1, count_band):
        parts.append(gram(shifted(flat, "band", step), flat))
    if count_band == 2:
        ordered = jnp.stack(
            [jnp.where(band == 0, parts[0], parts[1]), jnp.where(band == 0, parts[1], parts[0])]
        )
    else:
        ordered = jnp.stack(parts)[(band - jnp.arange(count_band)) % count_band]
    rows = count_band * band_width // count_elem
    pieces = ordered.reshape(count_elem, rows, band_width)
    landed = lax.all_to_all(pieces, "elem", 0, 0)
    summed = jnp.sum(landed.astype(jnp.float32), axis=0)
    margin = summed / jnp.float32(local_count * count_elem * block)
    return (current, margin)


def solution(mesh):
    in_specs = (
        P("elem", None, "band"),
        P("elem", None, "band"),
        P("elem", None, None),
        P("elem"),
        P("elem", None),
    )
    out_specs = (P("elem", None, "band"), P("elem", "band"))
    return jax.shard_map(
        on_device, mesh=mesh, in_specs=in_specs, out_specs=out_specs, check_vma=False
    )
```

```python
import jax
import jax.numpy as jnp
from jax import lax
from jax.experimental import pallas as pl
from jax.experimental.pallas import tpu as pltpu
from jax.sharding import PartitionSpec as P

GY = 16
DEGREES = 2

center_value = 0.3
spectral_half = 1.7

VM = pl.BlockSpec(memory_space=pltpu.VMEM)
SM = pl.BlockSpec(memory_space=pltpu.SMEM)
GRANT = pltpu.CompilerParams(vmem_limit_bytes=16 * 1024 * 1024)


def shifted(block, axis, distance):
    count = lax.axis_size(axis)
    return lax.ppermute(block, axis, [((i - distance) % count, i) for i in range(count)])


def own_bases(local_count, count_elem):
    myself = lax.axis_index("elem")
    before = jnp.where(myself == 0, count_elem - 1, myself - 1)
    after = jnp.where(myself == count_elem - 1, 0, myself + 1)
    return before * local_count, myself * local_count, after * local_count


def within(value, base, local_count):
    return (value >= base) & (value < base + local_count)


def send_lists(near, orders, local_count, bases):
    base_prev, _, base_next = bases
    to_next = jnp.int32(0)
    to_prev = jnp.int32(0)
    for i in range(local_count):
        lower = within(near[1, i], base_next, local_count)
        upper = within(near[0, i], base_prev, local_count)
        orders[jnp.where(lower, to_next, 2 * GY)] = i
        orders[jnp.where(upper, GY + to_prev, 2 * GY)] = i
        to_next = to_next + lower.astype(jnp.int32)
        to_prev = to_prev + upper.astype(jnp.int32)


def row_index(block, width):
    return lax.broadcasted_iota(jnp.int32, (block, width), 0)


def pack(values, sizes, near, count_elem):
    local_count, block, width = values.shape

    def body(near, sizes, values, to_next, to_prev, orders):
        bases = own_bases(local_count, count_elem)
        send_lists(near, orders, local_count, bases)
        rows = row_index(block, width)
        for s in range(GY):
            for out, at in ((to_next, orders[s]), (to_prev, orders[GY + s])):
                held = values[at].astype(jnp.float32)
                out[s] = jnp.where(rows < sizes[at], held, 0.0).astype(jnp.bfloat16)

    halo = jax.ShapeDtypeStruct((GY, block, width), jnp.bfloat16)
    return pl.pallas_call(
        body,
        name="pack",
        compiler_params=GRANT,
        in_specs=[SM, SM, VM],
        out_specs=[VM, VM],
        out_shape=[halo, halo],
        scratch_shapes=[pltpu.SMEM((2 * GY + 1,), jnp.int32)],
    )(near, sizes, values)


def tables(near, count_elem):
    local_count = near.shape[1]

    def body(near, pool_index, orders, slots, marks):
        bases = own_bases(local_count, count_elem)
        base_prev, base, base_next = bases
        send_lists(near, orders, local_count, bases)
        for j in range(2 * local_count):
            marks[j] = 0
        for i in range(local_count):
            upper = within(near[0, i], base_prev, local_count)
            lower = within(near[1, i], base_next, local_count)
            marks[jnp.where(upper, near[0, i] - base_prev, 2 * local_count)] = 1
            marks[jnp.where(lower, local_count + near[1, i] - base_next, 2 * local_count)] = 1
        from_prev = jnp.int32(local_count)
        from_next = jnp.int32(local_count + GY)
        for j in range(local_count):
            slots[j] = from_prev
            slots[local_count + j] = from_next
            from_prev = from_prev + marks[j]
            from_next = from_next + marks[local_count + j]
        for i in range(local_count):
            upper = within(near[0, i], base_prev, local_count)
            lower = within(near[1, i], base_next, local_count)
            far_prev = slots[jnp.where(upper, near[0, i] - base_prev, 0)]
            far_next = slots[jnp.where(lower, local_count + near[1, i] - base_next, 0)]
            pool_index[4 * i] = jnp.where(upper, far_prev, near[0, i] - base)
            pool_index[4 * i + 1] = jnp.where(lower, far_next, near[1, i] - base)
            pool_index[4 * i + 2] = near[2, i] - base
            pool_index[4 * i + 3] = near[3, i] - base

    return pl.pallas_call(
        body,
        name="tables",
        compiler_params=GRANT,
        in_specs=[SM],
        out_specs=[SM, SM],
        out_shape=[
            jax.ShapeDtypeStruct((4 * local_count,), jnp.int32),
            jax.ShapeDtypeStruct((2 * GY + 1,), jnp.int32),
        ],
        scratch_shapes=[
            pltpu.SMEM((2 * local_count,), jnp.int32),
            pltpu.SMEM((2 * local_count + 1,), jnp.int32),
        ],
    )(near)


def degree_step(pool_index, orders, sizes, current, previous, from_prev, from_next, h_blocks, last):
    local_count, block, width = current.shape

    def body(pool_index, orders, sizes, current, previous, from_prev, from_next, h_blocks, following, *rest):
        pool = rest[-1]
        rows = row_index(block, width)
        for i in range(local_count):
            held = current[i].astype(jnp.float32)
            pool[i] = jnp.where(rows < sizes[i], held, 0.0).astype(jnp.bfloat16)
        pool[local_count : local_count + GY] = from_prev[...]
        pool[local_count + GY :] = from_next[...]
        for i in range(local_count):
            own = pool[i]
            stacked = jnp.concatenate(
                [own] + [pool[pool_index[4 * i + k]] for k in range(4)], axis=0
            )
            applied = jnp.dot(h_blocks[i], stacked, preferred_element_type=jnp.float32)
            value = 2.0 / spectral_half * (
                applied - center_value * own.astype(jnp.float32)
            ) - previous[i].astype(jnp.float32)
            following[i] = jnp.where(rows < sizes[i], value, 0.0).astype(jnp.bfloat16)
        if not last:
            to_next, to_prev = rest[:2]
            for s in range(GY):
                to_next[s] = following[orders[s]]
                to_prev[s] = following[orders[GY + s]]

    whole = jax.ShapeDtypeStruct(current.shape, jnp.bfloat16)
    halo = jax.ShapeDtypeStruct((GY, block, width), jnp.bfloat16)
    outs = [whole] if last else [whole, halo, halo]
    return pl.pallas_call(
        body,
        name="degree_last" if last else "degree",
        compiler_params=GRANT,
        in_specs=[SM, SM, SM] + [VM] * 5,
        out_specs=[VM] * len(outs),
        out_shape=outs,
        scratch_shapes=[pltpu.VMEM((local_count + 2 * GY, block, width), jnp.bfloat16)],
    )(pool_index, orders, sizes, current, previous, from_prev, from_next, h_blocks)


def gram_pieces(blocks, count_elem, inner):
    depth, width = blocks[0].shape
    count_band = len(blocks)
    outer = count_elem // inner
    rows = count_band * width // count_elem

    def body(*refs):
        ins, outs, whole = refs[:count_band], refs[count_band:-1], refs[-1]
        band = lax.axis_index("band")
        place = lax.rem(lax.axis_index("elem"), inner)
        for step in range(count_band):
            source = lax.rem(band - step + count_band, count_band)
            whole[pl.ds(pl.multiple_of(source * width, width), width), :] = lax.dot_general(
                ins[step][...],
                ins[0][...],
                (((0,), (0,)), ((), ())),
                preferred_element_type=jnp.float32,
            )
        for d in range(inner):
            for o in range(outer):
                start = pl.multiple_of((o * inner + (place ^ d)) * rows, rows)
                outs[d][o] = whole[pl.ds(start, rows), :].astype(outs[d].dtype)

    piece = (outer, rows, width)
    return pl.pallas_call(
        body,
        name="gram",
        compiler_params=GRANT,
        in_specs=[VM] * count_band,
        out_specs=[VM] * inner,
        out_shape=[jax.ShapeDtypeStruct(piece, jnp.bfloat16 if d else jnp.float32) for d in range(inner)],
        scratch_shapes=[pltpu.VMEM((count_band * width, width), jnp.float32)],
    )(*blocks)


def sum_pieces(own, landed, inner):
    outer, rows, width = own.shape

    def body(*refs):
        ins, outs, whole = refs[: len(landed) + 1], refs[len(landed) + 1 : -1], refs[-1]
        place = lax.div(lax.axis_index("elem"), inner)
        total = ins[0][...]
        for ref in ins[1:]:
            total = total + ref[...].astype(jnp.float32)
        whole[...] = total
        for d in range(outer):
            outs[d][...] = whole[place ^ d].astype(outs[d].dtype)

    return pl.pallas_call(
        body,
        name="sum_inner",
        compiler_params=GRANT,
        in_specs=[VM] * (len(landed) + 1),
        out_specs=[VM] * outer,
        out_shape=[
            jax.ShapeDtypeStruct((rows, width), jnp.bfloat16 if d else jnp.float32) for d in range(outer)
        ],
        scratch_shapes=[pltpu.VMEM((outer, rows, width), jnp.float32)],
    )(own, *landed)


def last_sum(own, landed, divisor):
    def body(*refs):
        total = refs[0][...]
        for ref in refs[1:-1]:
            total = total + ref[...].astype(jnp.float32)
        refs[-1][...] = total / jnp.float32(divisor)

    return pl.pallas_call(
        body,
        name="sum_outer",
        compiler_params=GRANT,
        in_specs=[VM] * (len(landed) + 1),
        out_specs=VM,
        out_shape=jax.ShapeDtypeStruct(own.shape, jnp.float32),
    )(own, *landed)


def paired(block, flip):
    count = lax.axis_size("elem")
    return lax.ppermute(block, "elem", [(i, i ^ flip) for i in range(count)])


def on_device(y_current, y_previous, h_blocks, basis_sizes, neighbours):
    local_count, block, band_width = y_current.shape
    count_elem = lax.axis_size("elem")
    count_band = lax.axis_size("band")
    current, previous = y_current, y_previous
    neighbours = neighbours.T
    to_next, to_prev = pack(current, basis_sizes, neighbours, count_elem)
    pool_index, orders = tables(neighbours, count_elem)
    for degree in range(DEGREES):
        from_prev = shifted(to_next, "elem", 1)
        from_next = shifted(to_prev, "elem", -1)
        last = degree == DEGREES - 1
        result = degree_step(
            pool_index, orders, basis_sizes, current, previous, from_prev, from_next, h_blocks, last
        )
        previous = current
        current = result[0]
        if not last:
            to_next, to_prev = result[1:]
    flat = current.reshape(local_count * block, band_width)
    blocks = [flat] + [shifted(flat, "band", step) for step in range(1, count_band)]
    outer = 4
    inner = count_elem // outer
    pieces = gram_pieces(blocks, count_elem, inner)
    landed = [paired(pieces[d], d) for d in range(1, inner)]
    pieces = sum_pieces(pieces[0], landed, inner)
    landed = [paired(pieces[d], d * inner) for d in range(1, outer)]
    margin = last_sum(pieces[0], landed, local_count * count_elem * block)
    return (current, margin)


def solution(mesh):
    in_specs = (
        P("elem", None, "band"),
        P("elem", None, "band"),
        P("elem", None, None),
        P("elem"),
        P("elem", None),
    )
    out_specs = (P("elem", None, "band"), P("elem", "band"))
    return jax.shard_map(
        on_device, mesh=mesh, in_specs=in_specs, out_specs=out_specs, check_vma=False
    )
```

```python
import jax
import jax.numpy as jnp
from jax import lax
from jax.experimental import pallas as pl
from jax.experimental.pallas import tpu as pltpu
from jax.sharding import PartitionSpec as P

GY = 16
DEGREES = 2

center_value = 0.3
spectral_half = 1.7

VM = pl.BlockSpec(memory_space=pltpu.VMEM)
SM = pl.BlockSpec(memory_space=pltpu.SMEM)
GRANT = pltpu.CompilerParams(vmem_limit_bytes=16 * 1024 * 1024)


def shifted(block, axis, distance):
    count = lax.axis_size(axis)
    return lax.ppermute(block, axis, [((i - distance) % count, i) for i in range(count)])


def own_bases(local_count, count_elem):
    myself = lax.axis_index("elem")
    before = jnp.where(myself == 0, count_elem - 1, myself - 1)
    after = jnp.where(myself == count_elem - 1, 0, myself + 1)
    return before * local_count, myself * local_count, after * local_count


def within(value, base, local_count):
    return (value >= base) & (value < base + local_count)


def send_lists(near, orders, local_count, bases):
    base_prev, _, base_next = bases
    to_next = jnp.int32(0)
    to_prev = jnp.int32(0)
    for i in range(local_count):
        lower = within(near[1, i], base_next, local_count)
        upper = within(near[0, i], base_prev, local_count)
        orders[jnp.where(lower, to_next, 2 * GY)] = i
        orders[jnp.where(upper, GY + to_prev, 2 * GY)] = i
        to_next = to_next + lower.astype(jnp.int32)
        to_prev = to_prev + upper.astype(jnp.int32)


def row_index(block, width):
    return lax.broadcasted_iota(jnp.int32, (block, width), 0)


def pack(values, sizes, near, count_elem):
    local_count, block, width = values.shape

    def body(near, sizes, values, to_next, to_prev, orders):
        bases = own_bases(local_count, count_elem)
        send_lists(near, orders, local_count, bases)
        rows = row_index(block, width)
        for s in range(GY):
            for out, at in ((to_next, orders[s]), (to_prev, orders[GY + s])):
                held = values[at].astype(jnp.float32)
                out[s] = jnp.where(rows < sizes[at], held, 0.0).astype(jnp.bfloat16)

    halo = jax.ShapeDtypeStruct((GY, block, width), jnp.bfloat16)
    return pl.pallas_call(
        body,
        name="pack",
        compiler_params=GRANT,
        in_specs=[SM, SM, VM],
        out_specs=[VM, VM],
        out_shape=[halo, halo],
        scratch_shapes=[pltpu.SMEM((2 * GY + 1,), jnp.int32)],
    )(near, sizes, values)


def tables(near, sizes, h_blocks, previous, count_elem):
    local_count = near.shape[1]

    def body(near, sizes, h_blocks, previous, pool_index, orders, extents, h_held, held, slots, marks):
        h_held[...] = h_blocks[...]
        held[...] = previous[...]
        for i in range(local_count):
            extents[i] = sizes[i]
        bases = own_bases(local_count, count_elem)
        base_prev, base, base_next = bases
        send_lists(near, orders, local_count, bases)
        for j in range(2 * local_count):
            marks[j] = 0
        for i in range(local_count):
            upper = within(near[0, i], base_prev, local_count)
            lower = within(near[1, i], base_next, local_count)
            marks[jnp.where(upper, near[0, i] - base_prev, 2 * local_count)] = 1
            marks[jnp.where(lower, local_count + near[1, i] - base_next, 2 * local_count)] = 1
        from_prev = jnp.int32(local_count)
        from_next = jnp.int32(local_count + GY)
        for j in range(local_count):
            slots[j] = from_prev
            slots[local_count + j] = from_next
            from_prev = from_prev + marks[j]
            from_next = from_next + marks[local_count + j]
        for i in range(local_count):
            upper = within(near[0, i], base_prev, local_count)
            lower = within(near[1, i], base_next, local_count)
            far_prev = slots[jnp.where(upper, near[0, i] - base_prev, 0)]
            far_next = slots[jnp.where(lower, local_count + near[1, i] - base_next, 0)]
            pool_index[4 * i] = jnp.where(upper, far_prev, near[0, i] - base)
            pool_index[4 * i + 1] = jnp.where(lower, far_next, near[1, i] - base)
            pool_index[4 * i + 2] = near[2, i] - base
            pool_index[4 * i + 3] = near[3, i] - base

    return pl.pallas_call(
        body,
        name="tables",
        compiler_params=GRANT,
        in_specs=[SM, SM, VM, VM],
        out_specs=[SM, SM, SM, VM, VM],
        out_shape=[
            jax.ShapeDtypeStruct((4 * local_count,), jnp.int32),
            jax.ShapeDtypeStruct((2 * GY + 1,), jnp.int32),
            jax.ShapeDtypeStruct(sizes.shape, jnp.int32),
            jax.ShapeDtypeStruct(h_blocks.shape, h_blocks.dtype),
            jax.ShapeDtypeStruct(previous.shape, previous.dtype),
        ],
        scratch_shapes=[
            pltpu.SMEM((2 * local_count,), jnp.int32),
            pltpu.SMEM((2 * local_count + 1,), jnp.int32),
        ],
    )(near, sizes, h_blocks, previous)


def degree_step(pool_index, orders, sizes, current, previous, from_prev, from_next, h_blocks, last):
    local_count, block, width = current.shape

    def body(pool_index, orders, sizes, current, previous, from_prev, from_next, h_blocks, following, *rest):
        pool = rest[-1]
        rows = row_index(block, width)
        for i in range(local_count):
            held = current[i].astype(jnp.float32)
            pool[i] = jnp.where(rows < sizes[i], held, 0.0).astype(jnp.bfloat16)
        pool[local_count : local_count + GY] = from_prev[...]
        pool[local_count + GY :] = from_next[...]
        for i in range(local_count):
            own = pool[i]
            stacked = jnp.concatenate(
                [own] + [pool[pool_index[4 * i + k]] for k in range(4)], axis=0
            )
            applied = jnp.dot(h_blocks[i], stacked, preferred_element_type=jnp.float32)
            value = 2.0 / spectral_half * (
                applied - center_value * own.astype(jnp.float32)
            ) - previous[i].astype(jnp.float32)
            following[i] = jnp.where(rows < sizes[i], value, 0.0).astype(jnp.bfloat16)
        if last:
            rest[0][...] = following[...]
        else:
            to_next, to_prev = rest[:2]
            for s in range(GY):
                to_next[s] = following[orders[s]]
                to_prev[s] = following[orders[GY + s]]

    whole = jax.ShapeDtypeStruct(current.shape, jnp.bfloat16)
    halo = jax.ShapeDtypeStruct((GY, block, width), jnp.bfloat16)
    outs = [whole, whole] if last else [whole, halo, halo]
    return pl.pallas_call(
        body,
        name="degree_last" if last else "degree",
        compiler_params=GRANT,
        in_specs=[SM, SM, SM] + [VM] * 5,
        out_specs=[VM] * len(outs),
        out_shape=outs,
        scratch_shapes=[pltpu.VMEM((local_count + 2 * GY, block, width), jnp.bfloat16)],
    )(pool_index, orders, sizes, current, previous, from_prev, from_next, h_blocks)


def split_rows(whole, keep, send, bit):
    for g in range(keep.shape[0]):
        keep[g] = whole[2 * g + bit].astype(keep.dtype)
        send[g] = whole[2 * g + 1 - bit].astype(send.dtype)


def split_shapes(groups, rows, width):
    piece = (groups // 2, rows, width)
    return [jax.ShapeDtypeStruct(piece, jnp.float32), jax.ShapeDtypeStruct(piece, jnp.bfloat16)]


def gram_pieces(blocks, count_elem):
    depth, width = blocks[0].shape
    count_band = len(blocks)
    rows = count_band * width // count_elem
    per_band = width // rows

    def body(*refs):
        ins, keep, send, whole = refs[:count_band], *refs[count_band:]
        band = lax.axis_index("band")
        for step in range(count_band):
            source = lax.rem(band - step + count_band, count_band)
            product = lax.dot_general(
                ins[step][...],
                ins[0][...],
                (((0,), (0,)), ((), ())),
                preferred_element_type=jnp.float32,
            )
            for r in range(per_band):
                whole[source * per_band + r] = product[r * rows : (r + 1) * rows]
        split_rows(whole, keep, send, lax.rem(lax.axis_index("elem"), 2))

    return pl.pallas_call(
        body,
        name="gram",
        compiler_params=GRANT,
        in_specs=[VM] * count_band,
        out_specs=[VM, VM],
        out_shape=split_shapes(count_elem, rows, width),
        scratch_shapes=[pltpu.VMEM((count_elem, rows, width), jnp.float32)],
    )(*blocks)


def halve(kept, landed, flip):
    groups, rows, width = kept.shape

    def body(kept, landed, keep, send, whole):
        whole[...] = kept[...] + landed[...].astype(jnp.float32)
        split_rows(whole, keep, send, lax.rem(lax.div(lax.axis_index("elem"), flip), 2))

    return pl.pallas_call(
        body,
        name="halve",
        compiler_params=GRANT,
        in_specs=[VM, VM],
        out_specs=[VM, VM],
        out_shape=split_shapes(groups, rows, width),
        scratch_shapes=[pltpu.VMEM((groups, rows, width), jnp.float32)],
    )(kept, landed)


def last_sum(kept, landed, divisor):
    def body(kept, landed, out):
        out[...] = (kept[0] + landed[0].astype(jnp.float32)) / jnp.float32(divisor)

    return pl.pallas_call(
        body,
        name="last_sum",
        compiler_params=GRANT,
        in_specs=[VM, VM],
        out_specs=VM,
        out_shape=jax.ShapeDtypeStruct(kept.shape[1:], jnp.float32),
    )(kept, landed)


def paired(block, flip):
    count = lax.axis_size("elem")
    return lax.ppermute(block, "elem", [(i, i ^ flip) for i in range(count)])


def on_device(y_current, y_previous, h_blocks, basis_sizes, neighbours):
    local_count, block, band_width = y_current.shape
    count_elem = lax.axis_size("elem")
    count_band = lax.axis_size("band")
    current, previous = y_current, y_previous
    neighbours = neighbours.T
    to_next, to_prev = pack(current, basis_sizes, neighbours, count_elem)
    pool_index, orders, sizes, h_blocks, previous = tables(
        neighbours, basis_sizes, h_blocks, previous, count_elem
    )
    for degree in range(DEGREES):
        from_prev = shifted(to_next, "elem", 1)
        from_next = shifted(to_prev, "elem", -1)
        last = degree == DEGREES - 1
        result = degree_step(
            pool_index, orders, sizes, current, previous, from_prev, from_next, h_blocks, last
        )
        previous = current
        current = result[0]
        if not last:
            to_next, to_prev = result[1:]
    flat = result[1]
    flat = flat.reshape(local_count * block, band_width)
    blocks = [flat] + [shifted(flat, "band", step) for step in range(1, count_band)]
    keep, send = gram_pieces(blocks, count_elem)
    flip = 1
    landed = paired(send, flip)
    while 2 * flip < count_elem:
        flip *= 2
        keep, send = halve(keep, landed, flip)
        landed = paired(send, flip)
    margin = last_sum(keep, landed, local_count * count_elem * block)
    return (current, margin)


def solution(mesh):
    in_specs = (
        P("elem", None, "band"),
        P("elem", None, "band"),
        P("elem", None, None),
        P("elem"),
        P("elem", None),
    )
    out_specs = (P("elem", None, "band"), P("elem", "band"))
    return jax.shard_map(
        on_device, mesh=mesh, in_specs=in_specs, out_specs=out_specs, check_vma=False
    )
```

```python
import jax
import jax.numpy as jnp
from jax import lax
from jax.experimental import pallas as pl
from jax.experimental.pallas import tpu as pltpu
from jax.sharding import PartitionSpec as P

GY = 16
DEGREES = 2
CHUNKS = 2

center_value = 0.3
spectral_half = 1.7

VM = pl.BlockSpec(memory_space=pltpu.VMEM)
SM = pl.BlockSpec(memory_space=pltpu.SMEM)
GRANT = pltpu.CompilerParams(vmem_limit_bytes=16 * 1024 * 1024)


def shifted(block, axis, distance):
    count = lax.axis_size(axis)
    return lax.ppermute(block, axis, [((i - distance) % count, i) for i in range(count)])


def own_bases(local_count, count_elem):
    myself = lax.axis_index("elem")
    before = jnp.where(myself == 0, count_elem - 1, myself - 1)
    after = jnp.where(myself == count_elem - 1, 0, myself + 1)
    return before * local_count, myself * local_count, after * local_count


def within(value, base, local_count):
    return (value >= base) & (value < base + local_count)


def send_lists(near, orders, local_count, bases):
    base_prev, _, base_next = bases
    to_next = jnp.int32(0)
    to_prev = jnp.int32(0)
    for i in range(local_count):
        lower = within(near[1, i], base_next, local_count)
        upper = within(near[0, i], base_prev, local_count)
        orders[jnp.where(lower, to_next, 2 * GY)] = i
        orders[jnp.where(upper, GY + to_prev, 2 * GY)] = i
        to_next = to_next + lower.astype(jnp.int32)
        to_prev = to_prev + upper.astype(jnp.int32)


def row_index(block, width):
    return lax.broadcasted_iota(jnp.int32, (block, width), 0)


def pack(values, sizes, near, count_elem):
    local_count, block, width = values.shape

    part = width // CHUNKS

    def body(near, sizes, values, *rest):
        orders = rest[-1]
        bases = own_bases(local_count, count_elem)
        send_lists(near, orders, local_count, bases)
        rows = row_index(block, width)
        for s in range(GY):
            for way, at in enumerate((orders[s], orders[GY + s])):
                held = values[at].astype(jnp.float32)
                masked = jnp.where(rows < sizes[at], held, 0.0).astype(jnp.bfloat16)
                for c in range(CHUNKS):
                    rest[2 * c + way][s] = masked[:, c * part : (c + 1) * part]

    halo = jax.ShapeDtypeStruct((GY, block, part), jnp.bfloat16)
    return pl.pallas_call(
        body,
        name="pack",
        compiler_params=GRANT,
        in_specs=[SM, SM, VM],
        out_specs=[VM] * (2 * CHUNKS),
        out_shape=[halo] * (2 * CHUNKS),
        scratch_shapes=[pltpu.SMEM((2 * GY + 1,), jnp.int32)],
    )(near, sizes, values)


def tables(near, sizes, h_blocks, previous, count_elem):
    local_count = near.shape[1]

    def body(near, sizes, h_blocks, previous, pool_index, orders, extents, h_held, held, slots, marks):
        h_held[...] = h_blocks[...]
        held[...] = previous[...]
        for i in range(local_count):
            extents[i] = sizes[i]
        bases = own_bases(local_count, count_elem)
        base_prev, base, base_next = bases
        send_lists(near, orders, local_count, bases)
        for j in range(2 * local_count):
            marks[j] = 0
        for i in range(local_count):
            upper = within(near[0, i], base_prev, local_count)
            lower = within(near[1, i], base_next, local_count)
            marks[jnp.where(upper, near[0, i] - base_prev, 2 * local_count)] = 1
            marks[jnp.where(lower, local_count + near[1, i] - base_next, 2 * local_count)] = 1
        from_prev = jnp.int32(local_count)
        from_next = jnp.int32(local_count + GY)
        for j in range(local_count):
            slots[j] = from_prev
            slots[local_count + j] = from_next
            from_prev = from_prev + marks[j]
            from_next = from_next + marks[local_count + j]
        for i in range(local_count):
            upper = within(near[0, i], base_prev, local_count)
            lower = within(near[1, i], base_next, local_count)
            far_prev = slots[jnp.where(upper, near[0, i] - base_prev, 0)]
            far_next = slots[jnp.where(lower, local_count + near[1, i] - base_next, 0)]
            pool_index[4 * i] = jnp.where(upper, far_prev, near[0, i] - base)
            pool_index[4 * i + 1] = jnp.where(lower, far_next, near[1, i] - base)
            pool_index[4 * i + 2] = near[2, i] - base
            pool_index[4 * i + 3] = near[3, i] - base

    return pl.pallas_call(
        body,
        name="tables",
        compiler_params=GRANT,
        in_specs=[SM, SM, VM, VM],
        out_specs=[SM, SM, SM, VM, VM],
        out_shape=[
            jax.ShapeDtypeStruct((4 * local_count,), jnp.int32),
            jax.ShapeDtypeStruct((2 * GY + 1,), jnp.int32),
            jax.ShapeDtypeStruct(sizes.shape, jnp.int32),
            jax.ShapeDtypeStruct(h_blocks.shape, h_blocks.dtype),
            jax.ShapeDtypeStruct(previous.shape, previous.dtype),
        ],
        scratch_shapes=[
            pltpu.SMEM((2 * local_count,), jnp.int32),
            pltpu.SMEM((2 * local_count + 1,), jnp.int32),
        ],
    )(near, sizes, h_blocks, previous)


def degree_step(pool_index, orders, sizes, current, previous, from_prev, from_next, h_blocks, chunk, last):
    local_count, block, _ = current.shape
    width = from_prev.shape[2]

    def lanes(values):
        low = chunk * width if values.shape[2] > width else 0
        return slice(low, low + width)

    at_current, at_previous = lanes(current), lanes(previous)

    def body(pool_index, orders, sizes, current, previous, from_prev, from_next, h_blocks, following, *rest):
        pool = rest[-1]
        rows = row_index(block, width)
        for i in range(local_count):
            held = current[i, :, at_current].astype(jnp.float32)
            pool[i] = jnp.where(rows < sizes[i], held, 0.0).astype(jnp.bfloat16)
        pool[local_count : local_count + GY] = from_prev[...]
        pool[local_count + GY :] = from_next[...]
        for i in range(local_count):
            own = pool[i]
            stacked = jnp.concatenate(
                [own] + [pool[pool_index[4 * i + k]] for k in range(4)], axis=0
            )
            applied = jnp.dot(h_blocks[i], stacked, preferred_element_type=jnp.float32)
            value = 2.0 / spectral_half * (
                applied - center_value * own.astype(jnp.float32)
            ) - previous[i, :, at_previous].astype(jnp.float32)
            following[i] = jnp.where(rows < sizes[i], value, 0.0).astype(jnp.bfloat16)
        if not last:
            to_next, to_prev = rest[:2]
            for s in range(GY):
                to_next[s] = following[orders[s]]
                to_prev[s] = following[orders[GY + s]]

    whole = jax.ShapeDtypeStruct((local_count, block, width), jnp.bfloat16)
    halo = jax.ShapeDtypeStruct((GY, block, width), jnp.bfloat16)
    outs = [whole] if last else [whole, halo, halo]
    return pl.pallas_call(
        body,
        name="degree_last" if last else "degree",
        compiler_params=GRANT,
        in_specs=[SM, SM, SM] + [VM] * 5,
        out_specs=[VM] * len(outs),
        out_shape=outs,
        scratch_shapes=[pltpu.VMEM((local_count + 2 * GY, block, width), jnp.bfloat16)],
    )(pool_index, orders, sizes, current, previous, from_prev, from_next, h_blocks)


def split_rows(whole, keep, send, bit):
    for g in range(keep.shape[0]):
        keep[g] = whole[2 * g + bit].astype(keep.dtype)
        send[g] = whole[2 * g + 1 - bit].astype(send.dtype)


def split_shapes(groups, rows, width):
    piece = (groups // 2, rows, width)
    return [jax.ShapeDtypeStruct(piece, jnp.float32), jax.ShapeDtypeStruct(piece, jnp.bfloat16)]


def join(chunks):
    local_count, block, part = chunks[0].shape

    def body(*refs):
        for c in range(CHUNKS):
            refs[-1][:, :, c * part : (c + 1) * part] = refs[c][...]

    return pl.pallas_call(
        body,
        name="join",
        compiler_params=GRANT,
        in_specs=[VM] * CHUNKS,
        out_specs=VM,
        out_shape=jax.ShapeDtypeStruct((local_count, block, part * CHUNKS), jnp.bfloat16),
    )(*chunks)


def gram_pieces(blocks, count_elem):
    width = CHUNKS * blocks[0].shape[1]
    count_band = len(blocks) // CHUNKS
    rows = count_band * width // count_elem
    per_band = width // rows

    def body(*refs):
        ins, keep, send, whole = refs[: len(blocks)], *refs[len(blocks) :]
        sides = [
            jnp.concatenate([ref[...] for ref in ins[CHUNKS * k : CHUNKS * (k + 1)]], axis=1)
            for k in range(count_band)
        ]
        band = lax.axis_index("band")
        for step in range(count_band):
            source = lax.rem(band - step + count_band, count_band)
            product = lax.dot_general(
                sides[step],
                sides[0],
                (((0,), (0,)), ((), ())),
                preferred_element_type=jnp.float32,
            )
            for r in range(per_band):
                whole[source * per_band + r] = product[r * rows : (r + 1) * rows]
        split_rows(whole, keep, send, lax.rem(lax.axis_index("elem"), 2))

    return pl.pallas_call(
        body,
        name="gram",
        compiler_params=GRANT,
        in_specs=[VM] * len(blocks),
        out_specs=[VM, VM],
        out_shape=split_shapes(count_elem, rows, width),
        scratch_shapes=[pltpu.VMEM((count_elem, rows, width), jnp.float32)],
    )(*blocks)


def halve(kept, landed, flip):
    groups, rows, width = kept.shape

    def body(kept, landed, keep, send, whole):
        whole[...] = kept[...] + landed[...].astype(jnp.float32)
        split_rows(whole, keep, send, lax.rem(lax.div(lax.axis_index("elem"), flip), 2))

    return pl.pallas_call(
        body,
        name="halve",
        compiler_params=GRANT,
        in_specs=[VM, VM],
        out_specs=[VM, VM],
        out_shape=split_shapes(groups, rows, width),
        scratch_shapes=[pltpu.VMEM((groups, rows, width), jnp.float32)],
    )(kept, landed)


def last_sum(kept, landed, divisor):
    def body(kept, landed, out):
        out[...] = (kept[0] + landed[0].astype(jnp.float32)) / jnp.float32(divisor)

    return pl.pallas_call(
        body,
        name="last_sum",
        compiler_params=GRANT,
        in_specs=[VM, VM],
        out_specs=VM,
        out_shape=jax.ShapeDtypeStruct(kept.shape[1:], jnp.float32),
    )(kept, landed)


def paired(block, flip):
    count = lax.axis_size("elem")
    return lax.ppermute(block, "elem", [(i, i ^ flip) for i in range(count)])


def on_device(y_current, y_previous, h_blocks, basis_sizes, neighbours):
    local_count, block, band_width = y_current.shape
    count_elem = lax.axis_size("elem")
    count_band = lax.axis_size("band")
    neighbours = neighbours.T
    halos = pack(y_current, basis_sizes, neighbours, count_elem)
    halos = [halos[2 * c : 2 * c + 2] for c in range(CHUNKS)]
    pool_index, orders, sizes, h_blocks, y_previous = tables(
        neighbours, basis_sizes, h_blocks, y_previous, count_elem
    )
    current, previous = [y_current] * CHUNKS, [y_previous] * CHUNKS
    moved = []
    for degree in range(DEGREES):
        last = degree == DEGREES - 1
        arrived = [
            (shifted(to_next, "elem", 1), shifted(to_prev, "elem", -1)) for to_next, to_prev in halos
        ]
        for c in range(CHUNKS):
            result = degree_step(
                pool_index, orders, sizes, current[c], previous[c], *arrived[c], h_blocks, c, last
            )
            previous[c], current[c] = current[c], result[0]
            if last:
                flat = result[0].reshape(local_count * block, band_width // CHUNKS)
                moved.append([flat] + [shifted(flat, "band", step) for step in range(1, count_band)])
            else:
                halos[c] = result[1:]
    blocks = [moved[c][step] for step in range(count_band) for c in range(CHUNKS)]
    filtered = join(current)
    keep, send = gram_pieces(blocks, count_elem)
    flip = 1
    landed = paired(send, flip)
    while 2 * flip < count_elem:
        flip *= 2
        keep, send = halve(keep, landed, flip)
        landed = paired(send, flip)
    margin = last_sum(keep, landed, local_count * count_elem * block)
    return (filtered, margin)


def solution(mesh):
    in_specs = (
        P("elem", None, "band"),
        P("elem", None, "band"),
        P("elem", None, None),
        P("elem"),
        P("elem", None),
    )
    out_specs = (P("elem", None, "band"), P("elem", "band"))
    return jax.shard_map(
        on_device, mesh=mesh, in_specs=in_specs, out_specs=out_specs, check_vma=False
    )
```
